768 devices in a mesh: dp: 12 (over z), expert: 64 (over y, x, core).
Axes of the slice: x: 4, y: 8, z: 12, core: 2. Of those that a mesh axis runs over, the one named last changes fastest.
Arguments:
- tokens: bfloat16 [2048, 4096], P('expert'), may hold values from -6 to 6
- expert_ids: int32 [2048, 8], P('expert'), may hold values from 0 to 63, all different within a row; in each aligned block of 32 rows (0 to 31, 32 to 63, ...) at most 6 rows name the same one
- gate_ints: int32 [2048, 8], P('expert'), may hold values from 1 to 1024
- w_gate: bfloat16 [64, 4096, 1536], P('expert', None, 'dp'), may hold values from -0.09375 to 0.09375
- w_up: bfloat16 [64, 4096, 1536], P('expert', None, 'dp'), may hold values from -0.09375 to 0.09375
- w_down: bfloat16 [64, 1536, 4096], P('expert', 'dp'), may hold values from -0.15625 to 0.15625
Outputs:
- mixed: bfloat16 [2048, 4096], P('expert')
The draws below stay inside these ranges and needn't reach their ends.
Inputs may be any that keep to these rules, and one draw needn't show every extreme that they name: `expert_ids`: within the rows of one device each expert is named at most 6 times, and each row names 8 different experts.
All inputs are finite; a program needn't handle non-finite values.
Results may differ from the reference program's by a relative error of at most 0.017.
Values may be sent and summed in bfloat16 or wider, within the bound.
No kernel may reach another device: no remote copies, remote signals or barrier semaphores. Data moves between devices by JAX's collectives and lax.ppermute only.
A program may use at most 64 MiB of HBM per device.

```python
import math
import jax
import jax.numpy as jnp
import numpy as np
from jax import lax

D = 4096
FF = 1536
TOP = 8
TOK_DEV = 32
EXPERTS = 64
TOKENS = 2048
CAP = 6
N_DP = 12
N_EXPERT = 64


def touch_ends(entries, rng, least, high):
    place = [jax.random.randint(jax.random.fold_in(rng, axis), (), 0, length) for axis, length in enumerate(entries.shape)]
    longest = entries.shape.index(max(entries.shape))
    next_to = place[:longest] + [(place[longest] + 1) % entries.shape[longest]] + place[longest + 1:]
    return entries.at[tuple(place)].set(least).at[tuple(next_to)].set(high)


def shard_levels(key, shape, shards, least, high):
    def one(axis_at, shards_of):
        heights = jax.random.uniform(jax.random.fold_in(jax.random.fold_in(key, 6), axis_at), (shards_of,), jnp.float32, least / len(shards), high / len(shards))
        return jnp.repeat(jnp.exp(heights), shape[axis_at] // shards_of).reshape((-1,) + (1,) * (len(shape) - axis_at - 1))

    loudness = one(*shards[0])
    for cut in shards[1:]:
        loudness = loudness * one(*cut)
    return loudness


def assign_block(stream_key, own, number, rows, count, top, bound, skew):
    ranking = jax.random.permutation(stream_key, count)
    heavy_load, usual = portions_of(count, rows * top, bound, skew, True), portions_of(count, rows * top, bound, skew, False)
    places = jnp.arange(count)

    def named(sizes, offset_by):
        used = int((sizes > 0).sum())
        fixed = max(1, used // 4)
        shifted = fixed + (places - fixed + offset_by * (used - fixed)) % max(1, count - fixed)
        return jnp.zeros((count,), jnp.int32).at[ranking[jnp.where(places < fixed, places, shifted)]].set(jnp.asarray(sizes, jnp.int32))

    sizes = jnp.where(number % 4 == 0, named(heavy_load, number // 4), named(usual, number - number // 4 - 1))
    mixed = jax.random.permutation(jax.random.fold_in(own, 3), count)
    giver, sink = mixed[0:count // 2 * 2:2], mixed[1:count // 2 * 2:2]
    room = jnp.minimum(sizes[giver] - 1, bound - sizes[sink]) // 2
    room = jnp.where((giver == ranking[0]) | (sink == ranking[0]) | (sizes[sink] == 0), 0, jnp.maximum(room, 0))
    shifted = jax.random.randint(jax.random.fold_in(own, 4), (count // 2,), 0, 1 << 20) % (room + 1)
    sizes = sizes.at[giver].add(-shifted).at[sink].add(shifted)
    members = jnp.searchsorted(jnp.cumsum(sizes), jnp.arange(rows * top), side="right").astype(jnp.int32)
    listing = members.reshape(top, rows).T
    listing = listing[jax.random.permutation(jax.random.fold_in(own, 1), rows)]
    offset_by = jax.random.randint(jax.random.fold_in(own, 2), (rows, 1), 0, top)
    return jnp.take_along_axis(listing, (jnp.arange(top)[None, :] + offset_by) % top, axis=1)


def portions_of(number_of, total, reach, slope, full):
    portions = [(1 << 20) // math.isqrt(standing ** slope) + 1 for standing in range(1, number_of + 1)]
    largest = reach if full else min(reach, max(-(-total // number_of), total * portions[0] // sum(portions)))
    least = 1 if total - largest >= number_of - 1 else 0
    holding, rest = [largest] + [least] * (number_of - 1), total - largest - least * (number_of - 1)
    while rest > 0:
        candidates = [i for i in range(1, number_of) if holding[i] < largest] or [i for i in range(1, number_of) if holding[i] < reach]
        whole, budget = sum([portions[i] for i in candidates]), rest
        for i in candidates:
            addition = min(reach - holding[i], max(1, budget * portions[i] // whole), rest)
            holding[i] = holding[i] + addition
            rest = rest - addition
    return np.array(holding)


def noise(stream_key, shape, deviation, most, shards=(), kind=jnp.bfloat16):
    values = jax.random.normal(stream_key, shape, jnp.float32) * deviation
    if len(shards) > 0:
        values = shard_levels(stream_key, shape, shards, -0.22, 0.18) * values
    return jnp.clip(values, min=-most, max=most).astype(kind)


def setup_inputs(seed: int = 0) -> dict:
    arg_keys = jax.random.split(jax.random.key(seed), 7)
    tokens = noise(arg_keys[0], (TOKENS, D), 1.0, 6.0, ((0, 64),))
    expert_ids_keys = jax.random.split(jax.random.fold_in(arg_keys[1], 1), TOKENS // TOK_DEV)
    expert_ids_turns = jax.random.permutation(jax.random.fold_in(arg_keys[1], 3), TOKENS // TOK_DEV)
    expert_ids = jax.vmap(lambda own, number: assign_block(jax.random.fold_in(arg_keys[1], 2), own, number, TOK_DEV, EXPERTS, TOP, CAP, 2))(expert_ids_keys, expert_ids_turns).reshape((TOKENS, TOP))
    gate_ints = touch_ends(jax.random.randint(arg_keys[2], (TOKENS, TOP), 1, 1025), jax.random.fold_in(arg_keys[2], 1), 1, 1024).astype(jnp.int32)
    w_gate = noise(arg_keys[3], (EXPERTS, D, FF), D ** -0.5, 0.09375, ((0, 64), (2, 12)))
    w_up = noise(arg_keys[4], (EXPERTS, D, FF), D ** -0.5, 0.09375, ((0, 64), (2, 12)))
    w_down = noise(arg_keys[5], (EXPERTS, FF, D), FF ** -0.5, 0.15625, ((0, 64), (1, 12)))
    return dict(tokens=tokens, expert_ids=expert_ids, gate_ints=gate_ints, w_gate=w_gate, w_up=w_up, w_down=w_down)


def slots_of(expert_ids):
    blocks = expert_ids.reshape(N_EXPERT, TOK_DEV * TOP)
    onehot = (blocks[:, :, None] == jnp.arange(EXPERTS, dtype=jnp.int32)[None, None, :]).astype(jnp.int32)
    before = jnp.cumsum(onehot, axis=1) - onehot
    slot = jnp.sum(before * onehot, axis=2)
    return slot.reshape(TOKENS, TOP).astype(jnp.int32)


def expert_forward(packed):
    rows, gate_w, up_w, down_w = packed
    gate = jnp.dot(rows, gate_w, preferred_element_type=jnp.float32)
    up = jnp.dot(rows, up_w, preferred_element_type=jnp.float32)
    hidden = (jax.nn.silu(gate) * up).astype(jnp.bfloat16)
    split_hidden = hidden.reshape(rows.shape[0], N_DP, FF // N_DP).astype(jnp.float32)
    split_down = down_w.reshape(N_DP, FF // N_DP, D).astype(jnp.float32)
    partial_value = jnp.einsum("rsf,sfd->srd", split_hidden, split_down)
    partial_value = lax.optimization_barrier(partial_value.astype(jnp.bfloat16))
    return jnp.sum(partial_value.astype(jnp.float32), axis=0)


def reference(tokens, expert_ids, gate_ints, w_gate, w_up, w_down):
    slot = slots_of(expert_ids)
    block = (jnp.arange(TOKENS, dtype=jnp.int32) // TOK_DEV)[:, None]
    row_index = (block * CAP + slot).astype(jnp.int32)
    token_rows = jnp.broadcast_to(tokens[:, None, :], (TOKENS, TOP, D))
    buffer = jnp.zeros((EXPERTS, N_EXPERT * CAP, D), jnp.bfloat16)
    buffer = buffer.at[expert_ids.reshape(-1), row_index.reshape(-1)].set(token_rows.reshape(-1, D))
    expert_out = lax.map(expert_forward, (buffer, w_gate, w_up, w_down))
    picked = expert_out[expert_ids.reshape(-1), row_index.reshape(-1)].reshape(TOKENS, TOP, D)
    weights = gate_ints.astype(jnp.float32) / 1024.0
    mixed = jnp.sum(weights[:, :, None] * picked, axis=1)
    return mixed.astype(jnp.bfloat16)
```

```python
import jax
import jax.numpy as jnp
from jax import lax
from jax.sharding import PartitionSpec as P

BF16 = jnp.bfloat16
F32 = jnp.float32


def partner_pairs(n_dp, n_expert, step):
    pairs = []
    for p in range(n_dp):
        for e in range(n_expert):
            shift = e % 2
            other = ((((p - shift) % n_dp) ^ step) + shift) % n_dp
            pairs.append((p * n_expert + e, other * n_expert + e))
    return pairs


def exchange(x, pairs):
    return lax.ppermute(x, ("dp", "expert"), pairs)


def on_device(tokens, expert_ids, gate_ints, w_gate, w_up, w_down):
    n_dp, groups = lax.axis_size("dp"), lax.axis_size("expert")
    tok_rows, feature = tokens.shape
    top = expert_ids.shape[1]
    cap = min(tok_rows, max(2, 3 * tok_rows * top // (2 * groups)))
    rows = groups * cap
    half, quarter = feature // 2, feature // 4
    ff = w_gate.shape[2]
    p = lax.axis_index("dp")
    a, b = p % 2, (p // 2) % 2
    near = partner_pairs(n_dp, groups, 1)
    far = partner_pairs(n_dp, groups, 2)

    wg, wu, wd = w_gate[0], w_up[0], w_down[0]
    got_g = exchange(lax.dynamic_slice(wg, ((1 - a) * half, 0), (half, ff)), near)
    got_u = exchange(lax.dynamic_slice(wu, ((1 - a) * half, 0), (half, ff)), near)
    got_d = exchange(lax.dynamic_slice(wd, (0, (1 - a) * half), (ff, half)), near)
    own_g = lax.dynamic_slice(wg, (a * half, 0), (half, ff))
    own_u = lax.dynamic_slice(wu, (a * half, 0), (half, ff))
    own_d = lax.dynamic_slice(wd, (0, a * half), (ff, half))
    pair_d = jnp.concatenate([own_d, got_d], axis=0)
    got_d2 = exchange(
        lax.dynamic_slice(pair_d, (0, (1 - b) * quarter), (2 * ff, quarter)), far
    )
    keep_d = lax.dynamic_slice(pair_d, (0, b * quarter), (2 * ff, quarter))

    column = jnp.arange(rows, dtype=jnp.int32)
    named = expert_ids[:, :, None] == (column // cap)[None, None, :]
    member = jnp.any(named, axis=1)
    weight = jnp.sum(jnp.where(named, gate_ints[:, :, None], 0), axis=1)
    below = jnp.arange(tok_rows)[:, None] > jnp.arange(tok_rows)[None, :]
    slot = jnp.dot(below.astype(BF16), member.astype(BF16), preferred_element_type=F32)
    placed = member & (slot == (column % cap).astype(F32)[None, :])
    place = placed.astype(BF16)
    weight = jnp.where(placed, weight, 0)
    low = weight % 16
    mixing = jnp.concatenate([(weight - low).astype(BF16), low.astype(BF16)], axis=0)

    tok_half = lax.dynamic_slice(tokens, (0, a * half), (tok_rows, half))
    outgoing = lax.dot_general(
        place, tok_half, (((0,), (0,)), ((), ())), preferred_element_type=F32
    ).astype(BF16)

    def all_to_all(x):
        width = x.shape[1]
        chunk = x.reshape(groups, cap * width // 128, 128)
        chunk = lax.all_to_all(chunk, "expert", 0, 0, tiled=True)
        return chunk.reshape(rows, width)

    arrived = all_to_all(outgoing)
    w_all = jnp.concatenate([own_g, own_u, got_g, got_u], axis=1)
    part = jnp.dot(arrived, w_all, preferred_element_type=F32)
    part_out = jnp.concatenate([part[:, 2 * ff :], part[:, : 2 * ff]], axis=1)
    full = part + exchange(part_out.astype(BF16), near).astype(F32)
    hidden = jnp.concatenate(
        [
            jax.nn.silu(full[:, :ff]) * full[:, ff : 2 * ff],
            jax.nn.silu(full[:, 2 * ff : 3 * ff]) * full[:, 3 * ff :],
        ],
        axis=1,
    ).astype(BF16)
    hidden = jnp.concatenate([hidden, exchange(hidden, far)], axis=1)
    down = jnp.concatenate([keep_d, got_d2], axis=0)
    partial = jnp.dot(hidden, down, preferred_element_type=F32).astype(BF16)

    back = all_to_all(partial)
    both = jnp.dot(mixing, back, preferred_element_type=F32)
    local = (both[:tok_rows] + both[tok_rows:]) * (1.0 / 1024.0)
    tiles = lax.all_gather(local.astype(BF16), "dp")
    tiles = tiles.reshape(n_dp // 4, 4, tok_rows, quarter).astype(F32).sum(axis=0)
    mixed = jnp.concatenate([tiles[0], tiles[2], tiles[1], tiles[3]], axis=1)
    return mixed.astype(BF16)


def solution(mesh):
    return jax.shard_map(
        on_device,
        mesh=mesh,
        in_specs=(
            P("expert", None),
            P("expert", None),
            P("expert", None),
            P("expert", None, "dp"),
            P("expert", None, "dp"),
            P("expert", "dp", None),
        ),
        out_specs=P("expert", None),
        check_vma=False,
    )
```

```python
import jax
import jax.numpy as jnp
from jax import lax
from jax.sharding import PartitionSpec as P

BF16 = jnp.bfloat16
F32 = jnp.float32


def partner_pairs(n_dp, n_expert, step):
    pairs = []
    for p in range(n_dp):
        for e in range(n_expert):
            shift = e % 2
            other = ((((p - shift) % n_dp) ^ step) + shift) % n_dp
            pairs.append((p * n_expert + e, other * n_expert + e))
    return pairs


def exchange(x, pairs):
    return lax.ppermute(x, ("dp", "expert"), pairs)


def on_device(tokens, expert_ids, gate_ints, w_gate, w_up, w_down):
    n_dp, groups = lax.axis_size("dp"), lax.axis_size("expert")
    tok_rows, feature = tokens.shape
    top = expert_ids.shape[1]
    cap = min(tok_rows, max(2, 3 * tok_rows * top // (2 * groups)))
    rows = groups * cap
    half, quarter = feature // 2, feature // 4
    ff = w_gate.shape[2]
    p, e = lax.axis_index("dp"), lax.axis_index("expert")
    shift = e % 2
    place_in_quad = jnp.mod(p - shift, n_dp)
    first = place_in_quad % 2 == 0

    def plane(step):
        return jnp.mod((place_in_quad ^ step) + shift, n_dp)

    def half_of(q):
        return (q % 2) * half

    def quarter_of(q):
        return half_of(q) + ((q // 2) % 2) * quarter

    near = partner_pairs(n_dp, groups, 1)
    far = partner_pairs(n_dp, groups, 2)
    cross = partner_pairs(n_dp, groups, 3)

    ids, ints = expert_ids.T, gate_ints.T
    row = jnp.arange(rows, dtype=jnp.int32)[:, None]
    named = ids[:, None, :] == (row // cap)[None, :, :]
    member = jnp.any(named, axis=0)
    weight = jnp.sum(jnp.where(named, ints[:, None, :], 0), axis=0)
    above = jnp.arange(tok_rows)[:, None] < jnp.arange(tok_rows)[None, :]
    slot = jnp.dot(member.astype(BF16), above.astype(BF16), preferred_element_type=F32)
    placed = member & (slot == (row % cap).astype(F32))
    place = placed.astype(BF16)
    weight = jnp.where(placed, weight, 0)
    low = weight % 16
    mixing = jnp.concatenate([(weight - low).astype(BF16), low.astype(BF16)], axis=1)

    tok_half = lax.dynamic_slice(tokens, (0, half_of(p)), (tok_rows, half))
    outgoing = jnp.dot(place, tok_half, preferred_element_type=F32).astype(BF16)

    def all_to_all(x):
        width = x.shape[1]
        chunk = x.reshape(groups, cap * width // 128, 128)
        chunk = lax.all_to_all(chunk, "expert", 0, 0, tiled=True)
        return chunk.reshape(rows, width)

    arrived = all_to_all(outgoing)

    wg, wu, wd = w_gate[0], w_up[0], w_down[0]
    q_near, q_far, q_cross = plane(1), plane(2), plane(3)
    got_g = exchange(lax.dynamic_slice(wg, (half_of(q_near), 0), (half, ff)), near)
    got_u = exchange(lax.dynamic_slice(wu, (half_of(q_near), 0), (half, ff)), near)
    own_g = lax.dynamic_slice(wg, (half_of(p), 0), (half, ff))
    own_u = lax.dynamic_slice(wu, (half_of(p), 0), (half, ff))
    own_d, for_near, for_far, for_cross = [
        lax.dynamic_slice(wd, (0, quarter_of(q)), (ff, quarter))
        for q in (p, q_near, q_far, q_cross)
    ]
    got_near = exchange(for_near, near)
    got_far = exchange(for_far, far)
    got_cross = exchange(for_cross, cross)

    def in_order(mine, other, axis):
        return jnp.concatenate(
            [jnp.where(first, mine, other), jnp.where(first, other, mine)], axis=axis
        )

    up_down = in_order(
        jnp.concatenate([own_g, own_u], axis=1), jnp.concatenate([got_g, got_u], axis=1), 1
    )
    down = jnp.concatenate(
        [in_order(own_d, got_near, 0), in_order(got_far, got_cross, 0)], axis=0
    )
    arrived, up_down, down = lax.optimization_barrier((arrived, up_down, down))

    part = jnp.dot(arrived, up_down, preferred_element_type=F32)
    full = part + exchange(part.astype(BF16), near).astype(F32)
    hidden = jnp.concatenate(
        [
            jax.nn.silu(full[:, :ff]) * full[:, ff : 2 * ff],
            jax.nn.silu(full[:, 2 * ff : 3 * ff]) * full[:, 3 * ff :],
        ],
        axis=1,
    ).astype(BF16)
    hidden = jnp.concatenate([hidden, exchange(hidden, far)], axis=1)
    partial = jnp.dot(hidden, down, preferred_element_type=F32).astype(BF16)

    back = all_to_all(partial)
    both = lax.dot_general(
        mixing, back, (((0,), (0,)), ((), ())), preferred_element_type=F32
    )
    local = (both[:tok_rows] + both[tok_rows:]) * (1.0 / 1024.0)
    tiles = lax.all_gather(local.astype(BF16), "dp")
    tiles = tiles.reshape(n_dp // 4, 4, tok_rows, quarter).astype(F32).sum(axis=0)
    mixed = jnp.concatenate([tiles[0], tiles[2], tiles[1], tiles[3]], axis=1)
    return mixed.astype(BF16)


def solution(mesh):
    return jax.shard_map(
        on_device,
        mesh=mesh,
        in_specs=(
            P("expert", None),
            P("expert", None),
            P("expert", None),
            P("expert", None, "dp"),
            P("expert", None, "dp"),
            P("expert", "dp", None),
        ),
        out_specs=P("expert", None),
        check_vma=False,
    )
```

```python
import functools

import jax
import jax.numpy as jnp
from jax import lax
from jax.experimental import pallas as pl
from jax.experimental.pallas import tpu as pltpu
from jax.sharding import PartitionSpec as P

BF16 = jnp.bfloat16
F32 = jnp.float32


def near_of(p, core, n_dp):
    return ((p - core) % n_dp ^ 1) + core


def far_of(p, core, n_dp):
    return near_of(p, 1 - core, n_dp)


def pairs_of(n_dp, n_expert, target):
    pairs = []
    for p in range(n_dp):
        for e in range(n_expert):
            pairs.append((p * n_expert + e, target(p, e % 2) % n_dp * n_expert + e))
    return pairs


def exchange(x, pairs):
    return lax.ppermute(x, ("dp", "expert"), pairs)


def place_rows(cap, ids_ref, tok_ref, out_ref, used):
    top, tok_rows = ids_ref.shape

    def clear(i, carry):
        out_ref[i] = jnp.zeros(out_ref.shape[1:], out_ref.dtype)
        return carry

    lax.fori_loop(0, out_ref.shape[0], clear, 0, unroll=16)
    for e in range(used.shape[0]):
        used[e] = 0

    def one(t, carry):
        row = tok_ref[t]
        experts = [ids_ref[k, t] for k in range(top)]
        slots = [used[e] for e in experts]
        for e, slot in zip(experts, slots):
            out_ref[e * cap + slot] = row
            used[e] = slot + 1
        return carry

    lax.fori_loop(0, tok_rows, one, 0, unroll=4)


def dispatch_rows(ids, tok, groups, cap):
    return pl.pallas_call(
        functools.partial(place_rows, cap),
        out_shape=jax.ShapeDtypeStruct((groups * cap,) + tok.shape[1:], tok.dtype),
        in_specs=[
            pl.BlockSpec(memory_space=pltpu.SMEM),
            pl.BlockSpec(memory_space=pltpu.VMEM),
        ],
        out_specs=pl.BlockSpec(memory_space=pltpu.VMEM),
        scratch_shapes=[pltpu.SMEM((groups,), jnp.int32)],
        name="place_rows",
    )(ids, tok)


def on_device(tokens, expert_ids, gate_ints, w_gate, w_up, w_down):
    n_dp, groups = lax.axis_size("dp"), lax.axis_size("expert")
    tok_rows, feature = tokens.shape
    top = expert_ids.shape[1]
    cap = min(tok_rows, max(2, 3 * tok_rows * top // (2 * groups)))
    rows = groups * cap
    half, quarter = feature // 2, feature // 4
    ff = w_gate.shape[2]
    p = lax.axis_index("dp")
    core = lax.axis_index("expert") % 2

    def near_plane(q):
        return (jnp.mod(q - core, n_dp) ^ 1) + core

    def far_plane(q):
        return (jnp.mod(q - 1 + core, n_dp) ^ 1) + 1 - core

    near = pairs_of(n_dp, groups, lambda q, c: near_of(q, c, n_dp))
    far = pairs_of(n_dp, groups, lambda q, c: far_of(q, c, n_dp))
    cross = pairs_of(
        n_dp, groups, lambda q, c: far_of(near_of(q, c, n_dp) % n_dp, c, n_dp)
    )

    tok_half = lax.dynamic_slice(tokens, (0, p % 2 * half), (tok_rows, half))
    outgoing = dispatch_rows(
        expert_ids.T, tok_half.reshape(tok_rows, half // 128, 128), groups, cap
    )

    def all_to_all(chunk, width):
        chunk = chunk.reshape(groups, cap * width // 128, 128)
        chunk = lax.all_to_all(chunk, "expert", 0, 0, tiled=True)
        return chunk.reshape(rows, width)

    arrived = all_to_all(outgoing, half)

    wg, wu, wd = w_gate[0], w_up[0], w_down[0]

    def down_for(q):
        return lax.dynamic_slice(wd, (0, jnp.mod(q, 4) * quarter), (ff, quarter))

    def gate_up_for(q):
        at = (q % 2 * half, 0)
        return jnp.concatenate(
            [lax.dynamic_slice(w, at, (half, ff)) for w in (wg, wu)], axis=1
        )

    folds = quarter // (2 * ff)
    q_near, q_far = jnp.mod(near_plane(p), n_dp), jnp.mod(far_plane(p), n_dp)
    q_cross = jnp.mod(far_plane(q_near), n_dp)
    for_near = down_for(q_near)
    folded = [for_near[:, i * 2 * ff : (i + 1) * 2 * ff] for i in range(folds)]
    got = exchange(jnp.concatenate([gate_up_for(q_near)] + folded, axis=0), near)
    got_far = exchange(down_for(q_far), far)
    got_cross = exchange(down_for(q_cross), cross)
    got_near = jnp.concatenate(
        [got[half + i * ff : half + (i + 1) * ff] for i in range(folds)], axis=1
    )
    down = jnp.concatenate([down_for(p), got_near, got_far, got_cross], axis=0)
    own_gu = gate_up_for(p)
    arrived, own_gu, got_gu, down, late_ids, late_ints = lax.optimization_barrier(
        (arrived, own_gu, got[:half], down, expert_ids, gate_ints)
    )

    mine = jnp.dot(arrived, own_gu, preferred_element_type=F32)
    theirs = jnp.dot(arrived, got_gu, preferred_element_type=F32)
    other = exchange(jnp.concatenate([mine, theirs], axis=1).astype(BF16), near)

    row = jnp.arange(rows, dtype=jnp.int32)[:, None]
    named = late_ids.T[:, None, :] == (row // cap)[None, :, :]
    member = jnp.any(named, axis=0)
    weight = jnp.sum(jnp.where(named, late_ints.T[:, None, :], 0), axis=0)
    above = jnp.arange(tok_rows)[:, None] < jnp.arange(tok_rows)[None, :]
    slot = jnp.dot(member.astype(BF16), above.astype(BF16), preferred_element_type=F32)
    weight = jnp.where(member & (slot == (row % cap).astype(F32)), weight, 0)
    low = weight % 16
    mixing = jnp.concatenate([(weight - low).astype(BF16), low.astype(BF16)], axis=1)
    other, mixing = lax.optimization_barrier((other, mixing))

    def act(x, y):
        z = x + y.astype(F32)
        return (jax.nn.silu(z[:, :ff]) * z[:, ff:]).astype(BF16)

    hidden = jnp.concatenate(
        [act(mine, other[:, 2 * ff :]), act(theirs, other[:, : 2 * ff])], axis=1
    )
    hidden = jnp.concatenate([hidden, exchange(hidden, far)], axis=1)
    partial = jnp.dot(hidden, down, preferred_element_type=F32).astype(BF16)

    back = all_to_all(partial, quarter)
    both = lax.dot_general(
        mixing, back, (((0,), (0,)), ((), ())), preferred_element_type=F32
    )
    local = (both[:tok_rows] + both[tok_rows:]) * (1.0 / 1024.0)
    tiles = lax.all_gather(local.astype(BF16), "dp")
    tiles = tiles.reshape(n_dp // 4, 4, tok_rows, quarter).astype(F32).sum(axis=0)
    mixed = jnp.concatenate([tiles[i] for i in range(4)], axis=1)
    return mixed.astype(BF16)


def solution(mesh):
    return jax.shard_map(
        on_device,
        mesh=mesh,
        in_specs=(
            P("expert", None),
            P("expert", None),
            P("expert", None),
            P("expert", None, "dp"),
            P("expert", None, "dp"),
            P("expert", "dp", None),
        ),
        out_specs=P("expert", None),
        check_vma=False,
    )
```

```python
import functools

import jax
import jax.numpy as jnp
from jax import lax
from jax.experimental import pallas as pl
from jax.experimental.pallas import tpu as pltpu
from jax.sharding import PartitionSpec as P

BF16 = jnp.bfloat16
F32 = jnp.float32


def near_of(p, core, n_dp):
    return ((p - core) % n_dp ^ 1) + core


def far_of(p, core, n_dp):
    return near_of(p, 1 - core, n_dp)


def pairs_of(n_dp, n_expert, target):
    pairs = []
    for p in range(n_dp):
        for e in range(n_expert):
            pairs.append((p * n_expert + e, target(p, e % 2) % n_dp * n_expert + e))
    return pairs


def exchange(x, pairs):
    return lax.ppermute(x, ("dp", "expert"), pairs)


def gate_up_kernel(steps, x_ref, gate_ref, up_ref, got_ref, out_ref, acc):
    step = pl.program_id(0)
    ff = out_ref.shape[1] // 2

    @pl.when(step == 0)
    def _():
        acc[...] = jnp.zeros_like(acc)

    own = jnp.concatenate([gate_ref[...], up_ref[...]], axis=1)
    for i, w in enumerate((own, got_ref[...])):
        acc[i] += jnp.dot(x_ref[...], w, preferred_element_type=F32)

    @pl.when(step == steps - 1)
    def _():
        for i in range(2):
            gate, up = acc[i, :, :ff], acc[i, :, ff:]
            act = gate * (1.0 / (1.0 + jnp.exp(-gate))) * up
            out_ref[:, i * ff : (i + 1) * ff] = act.astype(out_ref.dtype)


def gate_up(x, gate, up, got):
    rows, depth = x.shape
    wide = got.shape[1]
    steps = 4
    block = depth // steps
    own = pl.BlockSpec((block, wide // 2), lambda i: (i, 0))
    return pl.pallas_call(
        functools.partial(gate_up_kernel, steps),
        grid=(steps,),
        out_shape=jax.ShapeDtypeStruct((rows, wide), BF16),
        in_specs=[
            pl.BlockSpec((rows, block), lambda i: (0, i)),
            own,
            own,
            pl.BlockSpec((block, wide), lambda i: (i, 0)),
        ],
        out_specs=pl.BlockSpec((rows, wide), lambda i: (0, 0)),
        scratch_shapes=[pltpu.VMEM((2, rows, wide), F32)],
        cost_estimate=pl.CostEstimate(
            flops=4 * rows * depth * wide,
            bytes_accessed=2 * depth * (rows + 2 * wide),
            transcendentals=rows * wide,
        ),
        compiler_params=pltpu.CompilerParams(
            dimension_semantics=("arbitrary",), vmem_limit_bytes=12 << 20
        ),
        name="gate_up",
    )(x, gate, up, got)


def on_device(tokens, expert_ids, gate_ints, w_gate, w_up, w_down):
    n_dp, groups = lax.axis_size("dp"), lax.axis_size("expert")
    tok_rows, feature = tokens.shape
    top = expert_ids.shape[1]
    cap = min(tok_rows, max(2, 3 * tok_rows * top // (2 * groups)))
    rows = groups * cap
    share, quarter = cap // 2, feature // 4
    ff = w_gate.shape[2]
    p = lax.axis_index("dp")
    core = lax.axis_index("expert") % 2

    def near_plane(q):
        return (jnp.mod(q - core, n_dp) ^ 1) + core

    def far_plane(q):
        return (jnp.mod(q - 1 + core, n_dp) ^ 1) + 1 - core

    near = pairs_of(n_dp, groups, lambda q, c: near_of(q, c, n_dp))
    far = pairs_of(n_dp, groups, lambda q, c: far_of(q, c, n_dp))
    cross = pairs_of(
        n_dp, groups, lambda q, c: far_of(near_of(q, c, n_dp) % n_dp, c, n_dp)
    )

    side = p % 2
    row = jnp.arange(groups * share, dtype=jnp.int32)[:, None]
    member = jnp.any(expert_ids.T[:, None, :] == (row // share)[None, :, :], axis=0)
    above = jnp.arange(tok_rows)[:, None] < jnp.arange(tok_rows)[None, :]
    slot = jnp.dot(member.astype(BF16), above.astype(BF16), preferred_element_type=F32)
    wanted = (row % share + side * share).astype(F32)
    place = (member & (slot == wanted)).astype(BF16)
    outgoing = jnp.dot(place, tokens, preferred_element_type=F32).astype(BF16)

    def all_to_all(chunk):
        return lax.all_to_all(chunk, "expert", 0, 0, tiled=True)

    arrived = all_to_all(outgoing.reshape(groups, share * feature // 128, 128))
    arrived = arrived.reshape(groups * share, feature)

    wd = w_down[0]

    def down_for(q):
        return lax.dynamic_slice(wd, (0, jnp.mod(q, 4) * quarter), (ff, quarter))

    q_near, q_far = near_plane(p), far_plane(p)
    q_cross = far_plane(jnp.mod(q_near, n_dp))
    got_gu = exchange(jnp.concatenate([w_gate[0], w_up[0]], axis=1), near)
    got_near = exchange(down_for(q_near), near)
    got_far = exchange(down_for(q_far), far)
    got_cross = exchange(down_for(q_cross), cross)
    down = jnp.concatenate([down_for(p), got_near, got_far, got_cross], axis=0)
    down, late_ids, late_ints = lax.optimization_barrier((down, expert_ids, gate_ints))

    row = jnp.arange(rows, dtype=jnp.int32)[:, None]
    named = late_ids.T[:, None, :] == (row // cap)[None, :, :]
    member = jnp.any(named, axis=0)
    weight = jnp.sum(jnp.where(named, late_ints.T[:, None, :], 0), axis=0)
    slot = jnp.dot(member.astype(BF16), above.astype(BF16), preferred_element_type=F32)
    weight = jnp.where(member & (slot == (row % cap).astype(F32)), weight, 0)
    low = weight % 16
    mixing = jnp.concatenate([(weight - low).astype(BF16), low.astype(BF16)], axis=1)
    arrived, got_gu, down, mixing = lax.optimization_barrier(
        (arrived, got_gu, down, mixing)
    )

    mine = gate_up(arrived, w_gate[0], w_up[0], got_gu)
    other = exchange(mine, near)
    other = jnp.concatenate([other[:, ff:], other[:, :ff]], axis=1)
    hidden = jnp.concatenate(
        [jnp.where(side == 0, mine, other), jnp.where(side == 0, other, mine)], axis=0
    )
    hidden = jnp.concatenate([hidden, exchange(hidden, far)], axis=1)
    partial = jnp.dot(hidden, down, preferred_element_type=F32).astype(BF16)

    chunk = partial.reshape(2, groups, share * quarter // 128, 128)
    chunk = jnp.concatenate([chunk[0], chunk[1]], axis=1)
    back = all_to_all(chunk).reshape(rows, quarter)
    both = lax.dot_general(
        mixing, back, (((0,), (0,)), ((), ())), preferred_element_type=F32
    )
    local = (both[:tok_rows] + both[tok_rows:]) * (1.0 / 1024.0)
    tiles = lax.all_gather(local.astype(BF16), "dp")
    tiles = tiles.reshape(n_dp // 4, 4, tok_rows, quarter).astype(F32).sum(axis=0)
    mixed = jnp.concatenate([tiles[i] for i in range(4)], axis=1)
    return mixed.astype(BF16)


def solution(mesh):
    return jax.shard_map(
        on_device,
        mesh=mesh,
        in_specs=(
            P("expert", None),
            P("expert", None),
            P("expert", None),
            P("expert", None, "dp"),
            P("expert", None, "dp"),
            P("expert", "dp", None),
        ),
        out_specs=P("expert", None),
        check_vma=False,
    )
```

```python
import jax
import jax.numpy as jnp
from jax import lax
from jax.sharding import PartitionSpec as P

BF16 = jnp.bfloat16
F32 = jnp.float32


def near_of(p, core, n_dp):
    return ((p - core) % n_dp ^ 1) + core


def far_of(p, core, n_dp):
    return near_of(p, 1 - core, n_dp)


def pairs_of(n_dp, n_expert, target):
    pairs = []
    for p in range(n_dp):
        for e in range(n_expert):
            pairs.append((p * n_expert + e, target(p, e % 2) % n_dp * n_expert + e))
    return pairs


def exchange(x, pairs):
    return lax.ppermute(x, ("dp", "expert"), pairs)


def on_device(tokens, expert_ids, gate_ints, w_gate, w_up, w_down):
    n_dp, groups = lax.axis_size("dp"), lax.axis_size("expert")
    tok_rows, feature = tokens.shape
    top = expert_ids.shape[1]
    cap = min(tok_rows, max(2, 3 * tok_rows * top // (2 * groups)))
    rows = groups * cap
    half, quarter = feature // 2, feature // 4
    ff = w_gate.shape[2]
    p = lax.axis_index("dp")
    core = lax.axis_index("expert") % 2

    def near_plane(q):
        return (jnp.mod(q - core, n_dp) ^ 1) + core

    def far_plane(q):
        return (jnp.mod(q - 1 + core, n_dp) ^ 1) + 1 - core

    near = pairs_of(n_dp, groups, lambda q, c: near_of(q, c, n_dp))
    far = pairs_of(n_dp, groups, lambda q, c: far_of(q, c, n_dp))
    cross = pairs_of(
        n_dp, groups, lambda q, c: far_of(near_of(q, c, n_dp) % n_dp, c, n_dp)
    )

    row = jnp.arange(rows, dtype=jnp.int32)[:, None]
    above = jnp.arange(tok_rows)[:, None] < jnp.arange(tok_rows)[None, :]

    def placement(ids):
        named = ids.T[:, None, :] == (row // cap)[None, :, :]
        member = jnp.any(named, axis=0)
        slot = jnp.dot(
            member.astype(BF16), above.astype(BF16), preferred_element_type=F32
        )
        return named, member & (slot == (row % cap).astype(F32))

    place = placement(expert_ids)[1].astype(BF16)
    tok_half = lax.dynamic_slice(tokens, (0, p % 2 * half), (tok_rows, half))
    outgoing = jnp.dot(place, tok_half, preferred_element_type=F32).astype(BF16)

    def all_to_all(chunk, width):
        chunk = chunk.reshape(groups, cap * width // 128, 128)
        chunk = lax.all_to_all(chunk, "expert", 0, 0, tiled=True)
        return chunk.reshape(rows, width)

    arrived = all_to_all(outgoing, half)

    wg, wu, wd = w_gate[0], w_up[0], w_down[0]

    def down_for(q):
        return lax.dynamic_slice(wd, (0, jnp.mod(q, 4) * quarter), (ff, quarter))

    def gate_up_for(q):
        at = (q % 2 * half, 0)
        return jnp.concatenate(
            [lax.dynamic_slice(w, at, (half, ff)) for w in (wg, wu)], axis=1
        )

    folds = quarter // (2 * ff)
    q_near, q_far = jnp.mod(near_plane(p), n_dp), jnp.mod(far_plane(p), n_dp)
    q_cross = jnp.mod(far_plane(q_near), n_dp)
    for_near = down_for(q_near)
    folded = [for_near[:, i * 2 * ff : (i + 1) * 2 * ff] for i in range(folds)]
    got = exchange(jnp.concatenate([gate_up_for(q_near)] + folded, axis=0), near)
    got_far = exchange(down_for(q_far), far)
    got_cross = exchange(down_for(q_cross), cross)
    got_near = jnp.concatenate(
        [got[half + i * ff : half + (i + 1) * ff] for i in range(folds)], axis=1
    )
    down = jnp.concatenate([down_for(p), got_near, got_far, got_cross], axis=0)
    own_gu = gate_up_for(p)
    arrived, own_gu, got_gu, down, late_ids, late_ints = lax.optimization_barrier(
        (arrived, own_gu, got[:half], down, expert_ids, gate_ints)
    )

    mine = jnp.dot(arrived, own_gu, preferred_element_type=F32)
    theirs = jnp.dot(arrived, got_gu, preferred_element_type=F32)
    other = exchange(jnp.concatenate([mine, theirs], axis=1).astype(BF16), near)

    named, placed = placement(late_ids)
    weight = jnp.sum(jnp.where(named, late_ints.T[:, None, :], 0), axis=0)
    weight = jnp.where(placed, weight, 0)
    low = weight % 16
    mixing = jnp.concatenate([(weight - low).astype(BF16), low.astype(BF16)], axis=1)
    other, mixing = lax.optimization_barrier((other, mixing))

    def act(x, y):
        z = x + y.astype(F32)
        return (jax.nn.silu(z[:, :ff]) * z[:, ff:]).astype(BF16)

    hidden = jnp.concatenate(
        [act(mine, other[:, 2 * ff :]), act(theirs, other[:, : 2 * ff])], axis=1
    )
    hidden = jnp.concatenate([hidden, exchange(hidden, far)], axis=1)
    partial = jnp.dot(hidden, down, preferred_element_type=F32).astype(BF16)

    back = all_to_all(partial, quarter)
    both = lax.dot_general(
        mixing, back, (((0,), (0,)), ((), ())), preferred_element_type=F32
    )
    local = (both[:tok_rows] + both[tok_rows:]) * (1.0 / 1024.0)
    tiles = lax.all_gather(local.astype(BF16), "dp")
    tiles = tiles.reshape(n_dp // 4, 4, tok_rows, quarter).astype(F32).sum(axis=0)
    mixed = jnp.concatenate([tiles[i] for i in range(4)], axis=1)
    return mixed.astype(BF16)


def solution(mesh):
    return jax.shard_map(
        on_device,
        mesh=mesh,
        in_specs=(
            P("expert", None),
            P("expert", None),
            P("expert", None),
            P("expert", None, "dp"),
            P("expert", None, "dp"),
            P("expert", "dp", None),
        ),
        out_specs=P("expert", None),
        check_vma=False,
    )
```

```python
import jax
import jax.numpy as jnp
from jax import lax
from jax.sharding import PartitionSpec as P

BF16 = jnp.bfloat16
F32 = jnp.float32


def near_of(p, core, n_dp):
    return ((p - core) % n_dp ^ 1) + core


def far_of(p, core, n_dp):
    return near_of(p, 1 - core, n_dp)


def pairs_of(n_dp, n_expert, target):
    pairs = []
    for p in range(n_dp):
        for e in range(n_expert):
            pairs.append((p * n_expert + e, target(p, e % 2) % n_dp * n_expert + e))
    return pairs


def exchange(x, pairs):
    return lax.ppermute(x, ("dp", "expert"), pairs)


def on_device(tokens, expert_ids, gate_ints, w_gate, w_up, w_down):
    n_dp, groups = lax.axis_size("dp"), lax.axis_size("expert")
    tok_rows, feature = tokens.shape
    top = expert_ids.shape[1]
    cap = min(tok_rows, max(2, 3 * tok_rows * top // (2 * groups)))
    rows = groups * cap
    half, quarter = feature // 2, feature // 4
    ff = w_gate.shape[2]
    p = lax.axis_index("dp")
    core = lax.axis_index("expert") % 2

    def near_plane(q):
        return (jnp.mod(q - core, n_dp) ^ 1) + core

    def far_plane(q):
        return (jnp.mod(q - 1 + core, n_dp) ^ 1) + 1 - core

    near = pairs_of(n_dp, groups, lambda q, c: near_of(q, c, n_dp))
    far = pairs_of(n_dp, groups, lambda q, c: far_of(q, c, n_dp))
    cross = pairs_of(
        n_dp, groups, lambda q, c: far_of(near_of(q, c, n_dp) % n_dp, c, n_dp)
    )

    row = jnp.arange(rows, dtype=jnp.int32)[:, None]
    above = jnp.arange(tok_rows)[:, None] < jnp.arange(tok_rows)[None, :]

    def placement(ids):
        named = ids.T[:, None, :] == (row // cap)[None, :, :]
        member = jnp.any(named, axis=0)
        slot = jnp.dot(
            member.astype(BF16), above.astype(BF16), preferred_element_type=F32
        )
        return named, member & (slot == (row % cap).astype(F32))

    place = placement(expert_ids)[1].astype(BF16)
    tok_half = lax.dynamic_slice(tokens, (0, p % 2 * half), (tok_rows, half))
    outgoing = jnp.dot(place, tok_half, preferred_element_type=F32).astype(BF16)

    def all_to_all(chunk, width):
        chunk = chunk.reshape(groups, cap * width // 128, 128)
        chunk = lax.all_to_all(chunk, "expert", 0, 0, tiled=True)
        return chunk.reshape(rows, width)

    arrived = all_to_all(outgoing, half)

    wg, wu, wd = w_gate[0], w_up[0], w_down[0]

    def down_for(q):
        return lax.dynamic_slice(wd, (0, jnp.mod(q, 4) * quarter), (ff, quarter))

    def gate_up_for(q):
        at = (q % 2 * half, 0)
        return jnp.concatenate(
            [lax.dynamic_slice(w, at, (half, ff)) for w in (wg, wu)], axis=1
        )

    q_near, q_far = jnp.mod(near_plane(p), n_dp), jnp.mod(far_plane(p), n_dp)
    q_cross = jnp.mod(far_plane(q_near), n_dp)
    got_gu = exchange(gate_up_for(q_near), near)
    got_near = exchange(down_for(q_near), near)
    got_far = exchange(down_for(q_far), far)
    got_cross = exchange(down_for(q_cross), cross)
    down = jnp.concatenate([down_for(p), got_near, got_far, got_cross], axis=0)
    weights = jnp.concatenate([gate_up_for(p), got_gu], axis=1)
    arrived, weights, down, late_ids, late_ints = lax.optimization_barrier(
        (arrived, weights, down, expert_ids, gate_ints)
    )

    parts = jnp.dot(arrived, weights, preferred_element_type=F32)
    other = exchange(parts.astype(BF16), near)
    mine, theirs = parts[:, : 2 * ff], parts[:, 2 * ff :]

    named, placed = placement(late_ids)
    weight = jnp.sum(jnp.where(named, late_ints.T[:, None, :], 0), axis=0)
    weight = jnp.where(placed, weight, 0)
    low = weight % 16
    mixing = jnp.concatenate([(weight - low).astype(BF16), low.astype(BF16)], axis=1)
    other, mixing = lax.optimization_barrier((other, mixing))

    def act(x, y):
        z = x + y.astype(F32)
        return (jax.nn.silu(z[:, :ff]) * z[:, ff:]).astype(BF16)

    hidden = jnp.concatenate(
        [act(mine, other[:, 2 * ff :]), act(theirs, other[:, : 2 * ff])], axis=1
    )
    hidden = jnp.concatenate([hidden, exchange(hidden, far)], axis=1)
    partial = jnp.dot(hidden, down, preferred_element_type=F32).astype(BF16)

    back = all_to_all(partial, quarter)
    both = lax.dot_general(
        mixing, back, (((0,), (0,)), ((), ())), preferred_element_type=F32
    )
    local = (both[:tok_rows] + both[tok_rows:]) * (1.0 / 1024.0)
    tiles = lax.all_gather(local.astype(BF16), "dp")
    tiles = tiles.reshape(n_dp // 4, 4, tok_rows, quarter).astype(F32).sum(axis=0)
    mixed = jnp.concatenate([tiles[i] for i in range(4)], axis=1)
    return mixed.astype(BF16)


def solution(mesh):
    return jax.shard_map(
        on_device,
        mesh=mesh,
        in_specs=(
            P("expert", None),
            P("expert", None),
            P("expert", None),
            P("expert", None, "dp"),
            P("expert", None, "dp"),
            P("expert", "dp", None),
        ),
        out_specs=P("expert", None),
        check_vma=False,
    )
```

```python
import jax
import jax.numpy as jnp
from jax import lax
from jax.sharding import PartitionSpec as P

BF16 = jnp.bfloat16
F32 = jnp.float32


def near_of(p, core, n_dp):
    return ((p - core) % n_dp ^ 1) + core


def far_of(p, core, n_dp):
    return near_of(p, 1 - core, n_dp)


def pairs_of(n_dp, n_expert, target):
    pairs = []
    for p in range(n_dp):
        for e in range(n_expert):
            pairs.append((p * n_expert + e, target(p, e % 2) % n_dp * n_expert + e))
    return pairs


def exchange(x, pairs):
    return lax.ppermute(x, ("dp", "expert"), pairs)


def on_device(tokens, expert_ids, gate_ints, w_gate, w_up, w_down):
    n_dp, groups = lax.axis_size("dp"), lax.axis_size("expert")
    tok_rows, feature = tokens.shape
    top = expert_ids.shape[1]
    cap = min(tok_rows, max(2, 3 * tok_rows * top // (2 * groups)))
    rows = groups * cap
    half, quarter = feature // 2, feature // 4
    ff = w_gate.shape[2]
    p = lax.axis_index("dp")
    core = lax.axis_index("expert") % 2

    def near_plane(q):
        return (jnp.mod(q - core, n_dp) ^ 1) + core

    def far_plane(q):
        return (jnp.mod(q - 1 + core, n_dp) ^ 1) + 1 - core

    near = pairs_of(n_dp, groups, lambda q, c: near_of(q, c, n_dp))
    far = pairs_of(n_dp, groups, lambda q, c: far_of(q, c, n_dp))
    cross = pairs_of(
        n_dp, groups, lambda q, c: far_of(near_of(q, c, n_dp) % n_dp, c, n_dp)
    )

    row = jnp.arange(rows, dtype=jnp.int32)[:, None]
    above = jnp.arange(tok_rows)[:, None] < jnp.arange(tok_rows)[None, :]

    def placement(ids):
        named = ids.T[:, None, :] == (row // cap)[None, :, :]
        member = jnp.any(named, axis=0)
        slot = jnp.dot(
            member.astype(BF16), above.astype(BF16), preferred_element_type=F32
        )
        return named, member & (slot == (row % cap).astype(F32))

    place = placement(expert_ids)[1].astype(BF16)
    tok_half = lax.dynamic_slice(tokens, (0, p % 2 * half), (tok_rows, half))
    outgoing = jnp.dot(place, tok_half, preferred_element_type=F32).astype(BF16)

    def all_to_all(chunk, width):
        chunk = chunk.reshape(groups, cap * width // 128, 128)
        chunk = lax.all_to_all(chunk, "expert", 0, 0, tiled=True)
        return chunk.reshape(rows, width)

    arrived = all_to_all(outgoing, half)

    wg, wu, wd = w_gate[0], w_up[0], w_down[0]

    def down_for(q):
        return lax.dynamic_slice(wd, (0, jnp.mod(q, 4) * quarter), (ff, quarter))

    def gate_up_for(q):
        at = (q % 2 * half, 0)
        return jnp.concatenate(
            [lax.dynamic_slice(w, at, (half, ff)) for w in (wg, wu)], axis=1
        )

    q_near, q_far = jnp.mod(near_plane(p), n_dp), jnp.mod(far_plane(p), n_dp)
    q_cross = jnp.mod(far_plane(q_near), n_dp)
    got_gu = exchange(gate_up_for(q_near), near)
    got_near = exchange(down_for(q_near), near)
    got_far = exchange(down_for(q_far), far)
    got_cross = exchange(down_for(q_cross), cross)
    down = jnp.concatenate([down_for(p), got_near, got_far, got_cross], axis=0)
    own_gu = gate_up_for(p)
    arrived, own_gu, got_gu, down, late_ids, late_ints = lax.optimization_barrier(
        (arrived, own_gu, got_gu, down, expert_ids, gate_ints)
    )

    weights = jnp.concatenate([own_gu, got_gu], axis=1)
    parts = jnp.dot(arrived, weights, preferred_element_type=F32)
    other = exchange(parts.astype(BF16), near)
    mine, theirs = parts[:, : 2 * ff], parts[:, 2 * ff :]

    named, placed = placement(late_ids)
    weight = jnp.sum(jnp.where(named, late_ints.T[:, None, :], 0), axis=0)
    weight = jnp.where(placed, weight, 0)
    low = weight % 16
    mixing = jnp.concatenate([(weight - low).astype(BF16), low.astype(BF16)], axis=1)
    other, mixing = lax.optimization_barrier((other, mixing))

    def act(x, y):
        z = x + y.astype(F32)
        return (jax.nn.silu(z[:, :ff]) * z[:, ff:]).astype(BF16)

    hidden = jnp.concatenate(
        [act(mine, other[:, 2 * ff :]), act(theirs, other[:, : 2 * ff])], axis=1
    )
    hidden = jnp.concatenate([hidden, exchange(hidden, far)], axis=1)
    partial = jnp.dot(hidden, down, preferred_element_type=F32).astype(BF16)

    back = all_to_all(partial, quarter)
    both = lax.dot_general(
        mixing, back, (((0,), (0,)), ((), ())), preferred_element_type=F32
    )
    local = (both[:tok_rows] + both[tok_rows:]) * (1.0 / 1024.0)
    tiles = lax.all_gather(local.astype(BF16), "dp")
    tiles = tiles.reshape(n_dp // 4, 4, tok_rows, quarter).astype(F32).sum(axis=0)
    mixed = jnp.concatenate([tiles[i] for i in range(4)], axis=1)
    return mixed.astype(BF16)


def solution(mesh):
    return jax.shard_map(
        on_device,
        mesh=mesh,
        in_specs=(
            P("expert", None),
            P("expert", None),
            P("expert", None),
            P("expert", None, "dp"),
            P("expert", None, "dp"),
            P("expert", "dp", None),
        ),
        out_specs=P("expert", None),
        check_vma=False,
    )
```
